32 devices in a mesh: coil: 4 (over y, core), spoke: 8 (over z, x).
Axes of the slice: x: 2, y: 2, z: 4, core: 2. Of those that a mesh axis runs over, the one named last changes fastest.
Arguments:
- kdata: bfloat16 [64, 8, 2, 64, 256], P('spoke', 'coil'), may hold values from -6 to 6
- coords: float32 [64, 2, 256], P('spoke'), may hold values from 0 to 256, as said below
- foot_offset: int32 [64, 8], P('spoke'), may hold values from 0 to 224, as said below
- live_count: int32 [8], P('spoke'), may hold values from 1 to 8, 48 in all
- dcf_table: float32 [129], replicated, may hold values from 0.1 to 4
- dcf_index: int32 [64, 256], P('spoke'), may hold values from 0 to 128
- slab_owner: int32 [8], replicated, may hold values from 0 to 7, each once
Outputs:
- coil_images: float32 [256, 8, 2, 64, 256], P('spoke', 'coil')
- combined: float32 [256, 64, 256], P('spoke', 'coil')
The draws below stay inside these ranges and needn't reach their ends.
Inputs may be any that keep to these rules, and one draw needn't show every extreme that they name: coords[p, 0, s] lies between s and s + 1; coords[p, 1, s] lies between foot_offset[p, s // 32] + 3 and foot_offset[p, s // 32] + 29. `foot_offset`: for each block of 8 spoke slots (the slots of one device index of spoke) and each slab, the offsets lie between b and b + 16, where b is the smallest of them, and both ends are taken; b <= 208.
All inputs are finite; a program needn't handle non-finite values. No bound on the sum of `live_count` on one device may be relied on, other than what follows from the above.
Results may differ from the reference program's by a relative error of at most 0.0028.
Values may be sent and summed in bfloat16 or wider, within the bound.
A program may use at most 128 MiB of HBM per device.

```python
import math
import jax
import jax.numpy as jnp
import numpy as np
from jax import lax

GRID = 256
KZ = 64
S_DEV = 8
FW = 32
UW = 48
HALO = 4
COILS = 8
SPOKES = 64
SAMP = 256
NW = 129
N_SPOKE = 8


def footprint_layout(key):
    slab_rows = GRID // N_SPOKE
    slope_key, relative_key, pick_key = jax.random.split(jax.random.fold_in(key, 71), 3)
    slopes = jax.random.randint(slope_key, (N_SPOKE,), -64, 65)
    centres = jnp.arange(N_SPOKE, dtype=jnp.int32) * slab_rows + slab_rows // 2 - GRID // 2
    window_base = GRID // 2 + centres[None, :] * slopes[:, None] // 64 - UW // 2
    window_base = jnp.clip(window_base, 0, GRID - UW)
    relative = jax.random.randint(relative_key, (N_SPOKE, S_DEV, N_SPOKE), 0, UW - FW + 1)
    shuffled = jax.vmap(lambda subkey: jax.random.permutation(subkey, S_DEV))(jax.random.split(pick_key, N_SPOKE))
    low_slot = shuffled[:, 0]
    high_slot = shuffled[:, 1]
    slot_ids = jnp.arange(S_DEV, dtype=jnp.int32)
    relative = jnp.where(slot_ids[None, :, None] == low_slot[:, None, None], 0, relative)
    relative = jnp.where(slot_ids[None, :, None] == high_slot[:, None, None], UW - FW, relative)
    layout = window_base[:, None, :] + relative
    return layout.reshape(N_SPOKE * S_DEV, N_SPOKE).astype(jnp.int32)


def draw_foot_offset(key, part):
    return footprint_layout(key)


def draw_coords(key, part):
    offsets = footprint_layout(key)
    slab_rows = GRID // N_SPOKE
    first_key, second_key = jax.random.split(jax.random.fold_in(key, 5))
    sample = jnp.arange(GRID, dtype=jnp.int32)
    reach = FW // 2 - 3
    along = jax.random.uniform(first_key, (SPOKES, GRID), jnp.float32, -0.5, 0.5)
    across = jax.random.uniform(second_key, (SPOKES, GRID), jnp.float32, -reach, reach)
    row_coord = sample.astype(jnp.float32)[None, :] + 0.5 + along
    start_cols = offsets[:, sample // slab_rows].astype(jnp.float32)
    col_coord = start_cols + FW / 2 + across
    return jnp.stack([row_coord, col_coord], axis=1).astype(jnp.float32)


def draw_dcf_index(key, part):
    sample = jnp.arange(GRID, dtype=jnp.int32)
    radial = jnp.abs(2 * sample + 1 - GRID) // 2
    jitter = jax.random.randint(jax.random.fold_in(key, 13), (SPOKES, GRID), 0, 2)
    return jnp.minimum(radial[None, :] + jitter, NW - 1).astype(jnp.int32)


def steps_of(stream_key, extent, cuts, smallest, high):
    level, own = 1.0, jax.random.fold_in(stream_key, 6)
    for axis_at, shards_of in cuts:
        heights = jnp.exp(jax.random.uniform(jax.random.fold_in(own, axis_at), (shards_of,), jnp.float32, smallest / len(cuts), high / len(cuts)))
        level = level * jnp.repeat(heights, extent[axis_at] // shards_of).reshape([-1 if axis == axis_at else 1 for axis in range(len(extent))])
    return level


def profile(amount, total, most, slope):
    loads = [(1 << 20) // math.isqrt(rank ** slope) + 1 for rank in range(2, amount + 1)]
    rest, holding = total - most - (amount - 1), [1] * (amount - 1)
    while rest > 0:
        movable = [i for i in range(amount - 1) if holding[i] < most]
        pool, remaining = sum([loads[i] for i in movable]), rest
        for i in movable:
            more = min(most - holding[i], max(1, remaining * loads[i] // pool), rest)
            holding[i] = holding[i] + more
            rest = rest - more
    return np.array([most] + holding)


def uneven(own_key, count, total, most, slope):
    if count == 2:
        one = jax.random.randint(own_key, (), max(1, total - most), min(most, total - 1) + 1)
        return jnp.stack([one, total - one])
    sizes = jnp.asarray(profile(count, total, most, slope), jnp.int32)
    couples = (count - 1) // 2
    source_of, taker = sizes[1:1 + 2 * couples:2], sizes[2:2 + 2 * couples:2]
    slack = jnp.minimum(source_of - 1, most - taker)
    passed = jax.random.randint(jax.random.fold_in(own_key, 1), (couples,), 0, 1 << 20) % (slack + 1)
    sizes = sizes.at[1:1 + 2 * couples:2].set(source_of - passed).at[2:2 + 2 * couples:2].set(taker + passed)
    return sizes[jax.random.permutation(jax.random.fold_in(own_key, 2), count)]


def normal_values(stream_key, shape, deviation, most, shards=(), held_as=jnp.bfloat16):
    drawn = jax.random.normal(stream_key, shape, jnp.float32) * deviation
    if len(shards) > 0:
        drawn = steps_of(stream_key, shape, shards, -0.22, 0.18) * drawn
    return jnp.clip(drawn, min=-most, max=most).astype(held_as)


def setup_inputs(seed: int = 0) -> dict:
    arg_keys = jax.random.split(jax.random.key(seed), 8)
    return {
        "kdata": normal_values(arg_keys[0], (SPOKES, COILS, 2, KZ, SAMP), 1.0, 6.0, ((0, 8), (1, 4))),
        "coords": draw_coords(jax.random.fold_in(arg_keys[7], 71), 0),
        "foot_offset": draw_foot_offset(jax.random.fold_in(arg_keys[7], 71), 0),
        "live_count": uneven(arg_keys[3], N_SPOKE, (3 * S_DEV * N_SPOKE) // 4, S_DEV, 2).astype(jnp.int32),
        "dcf_table": jnp.clip(jnp.exp(jax.random.uniform(arg_keys[4], (NW,), jnp.float32, math.log(0.1), math.log(4.0))), 0.1, 4.0),
        "dcf_index": draw_dcf_index(jax.random.fold_in(arg_keys[7], 71), 0),
        "slab_owner": jax.random.permutation(arg_keys[6], N_SPOKE).astype(jnp.int32),
    }


def kernel(distance):
    inner = jnp.maximum(1.0 - distance * distance * 0.25, 0.0)
    return inner * inner

def reference(kdata, coords, foot_offset, live_count, dcf_table, dcf_index, slab_owner):
    spokes = kdata.shape[0]
    slab_rows = GRID // N_SPOKE
    block_len = slab_rows + 2 * HALO
    columns = COILS * 2 * KZ
    slot_index = jnp.arange(spokes, dtype=jnp.int32)
    live_flag = (slot_index % S_DEV < jnp.repeat(live_count, S_DEV)).astype(jnp.float32)
    density = dcf_table[dcf_index] * live_flag[:, None]
    values = kdata.reshape(spokes, columns, SAMP)

    def one_slab(slab_index):
        position = (slab_index * slab_rows - HALO + jnp.arange(block_len, dtype=jnp.int32)).astype(jnp.int32)
        inside = (position >= 0) & (position < SAMP)
        clipped = jnp.clip(position, 0, SAMP - 1).astype(jnp.int32)
        row_coord = coords[:, 0, :][:, clipped]
        col_coord = coords[:, 1, :][:, clipped]
        block_density = jnp.where(inside[None, :], density[:, clipped], 0.0)
        sample_block = jnp.where(inside[None, None, :], values[:, :, clipped], jnp.zeros((), kdata.dtype)).astype(jnp.float32)
        rows = (slab_index * slab_rows + jnp.arange(slab_rows, dtype=jnp.int32)).astype(jnp.float32)
        row_weight = block_density[:, :, None] * kernel(rows[None, None, :] + 0.5 - row_coord[:, :, None])
        offsets = jnp.take(foot_offset, slab_index, axis=1).astype(jnp.int32)
        cell_cols = offsets[:, None] + jnp.arange(FW, dtype=jnp.int32)[None, :]
        col_weight = kernel(cell_cols.astype(jnp.float32)[:, None, :] + 0.5 - col_coord[:, :, None])
        weights = (row_weight[..., None] * col_weight[:, :, None, :]).astype(jnp.bfloat16)
        weights = lax.optimization_barrier(weights).astype(jnp.float32)
        weights = weights.reshape(N_SPOKE, S_DEV, block_len, slab_rows * FW)
        grouped = sample_block.reshape(N_SPOKE, S_DEV, columns, block_len)
        cell_groups = cell_cols.reshape(N_SPOKE, S_DEV, FW)

        def add_group(running, group_data):
            group_values, group_weights, cell_index = group_data
            tile_sums = jnp.einsum('pcq,pqk->cpk', group_values, group_weights)
            tile_sums = tile_sums.reshape(columns, S_DEV, slab_rows, FW).transpose(0, 2, 1, 3)
            return (running.at[:, :, cell_index].add(tile_sums), None)
        start = jnp.zeros((columns, slab_rows, GRID), jnp.float32)
        slab_grid, _ = lax.scan(add_group, start, (grouped, weights, cell_groups))
        layered = slab_grid.reshape(COILS, 2, KZ, slab_rows, GRID)
        spectrum = layered[:, 0] + 1j * layered[:, 1]
        image = jnp.fft.ifft2(spectrum, axes=(1, 3), norm='ortho')
        images = jnp.stack([jnp.real(image), jnp.imag(image)], axis=1).astype(jnp.float32)
        images = images.transpose(3, 0, 1, 2, 4)
        power_sum = lax.optimization_barrier(jnp.sum(images * images, axis=(1, 2)))
        return (images, power_sum)
    all_images, all_power = lax.map(one_slab, jnp.arange(N_SPOKE, dtype=jnp.int32))
    coil_images = all_images[slab_owner].reshape(GRID, COILS, 2, KZ, GRID)
    combined = jnp.sqrt(all_power[slab_owner]).reshape(GRID, KZ, GRID)
    return (coil_images, combined)
```

```python
import functools
import math

import jax
import jax.numpy as jnp
import numpy as np
from jax import lax
from jax.experimental import pallas as pl
from jax.experimental.pallas import tpu as pltpu
from jax.sharding import PartitionSpec as P

FW = 32
REACH = 2
ROWS_STEP = 4


def kernel(distance):
    inner = jnp.maximum(1.0 - distance * distance * 0.25, 0.0)
    return inner * inner


def inverse_matrix(length):
    counter = np.arange(length)
    phase = 2.0 * np.pi / length * (counter[:, None] * counter[None, :] % length)
    cosine = np.cos(phase) / math.sqrt(length)
    sine = np.sin(phase) / math.sqrt(length)
    return np.block([[cosine, sine], [-sine, cosine]])


def two_terms(table):
    high = table.astype(jnp.bfloat16)
    low = (table - high.astype(np.float64)).astype(jnp.bfloat16)
    return high, low


def slab_kernel(
    slab_ref, value_ref, geometry_ref, high_ref, low_ref, image_ref, power_ref, turned_ref, col_ref, row_ref, *, group
):
    step = pl.program_id(0)
    rows_step, coil_dev, _, kz_len, grid_len = image_ref.shape
    slab_rows, depth = row_ref.shape

    @pl.when(step == 0)
    def _():
        first_row = slab_ref[0] * slab_rows
        chunk = 2 * group
        for start in range(0, depth, chunk):
            part = slice(start, start + chunk)
            turned_ref[:, part] = value_ref[part, :].T
            geometry = geometry_ref[:, part]
            cells = lax.broadcasted_iota(jnp.int32, (grid_len, chunk), 0).astype(jnp.float32)
            begin = geometry[3:4]
            covered = (cells >= begin) & (cells < begin + FW)
            col_ref[:, part] = jnp.where(covered, kernel(cells + 0.5 - geometry[1:2]), 0.0)
            rows = (first_row + lax.broadcasted_iota(jnp.int32, (slab_rows, chunk), 0)).astype(jnp.float32)
            row_ref[:, part] = geometry[2:3] * kernel(rows + 0.5 - geometry[0:1])

    span = (2 + 2 * REACH) * group
    pieces = []
    for pair in range(rows_step // 2):
        row = step * rows_step + 2 * pair
        lanes = pl.ds(pl.multiple_of(row * group, 128), span)
        values = turned_ref[:, lanes]
        columns = col_ref[:, lanes]
        for half in range(2):
            weight = (row_ref[pl.ds(row + half, 1), lanes] * columns).astype(jnp.bfloat16)
            cells = lax.dot_general(
                values, weight, (((1,), (1,)), ((), ())), preferred_element_type=jnp.float32
            ).astype(jnp.bfloat16)
            for coil in range(coil_dev):
                base = coil * 2 * kz_len
                pieces.append(
                    jnp.concatenate([cells[base : base + kz_len], cells[base + kz_len : base + 2 * kz_len]], axis=1)
                )
    stacked = jnp.concatenate(pieces, axis=0)
    out = jnp.dot(stacked, high_ref[...], preferred_element_type=jnp.float32)
    out = out + jnp.dot(stacked, low_ref[...], preferred_element_type=jnp.float32)
    for row in range(rows_step):
        power = jnp.zeros((kz_len, grid_len), jnp.float32)
        for coil in range(coil_dev):
            base = (row * coil_dev + coil) * kz_len
            for part in range(2):
                image = out[base : base + kz_len, part * grid_len : (part + 1) * grid_len]
                image_ref[row, coil, part] = image
                power = power + image * image
        power_ref[row] = power.astype(power_ref.dtype)


def on_device(depth_tables, column_tables, kdata, coords, foot_offset, live_count, dcf_table, dcf_index, slab_owner):
    slot_count, coil_dev, part_count, kz_len, grid_len = kdata.shape
    slab_count = lax.axis_size("spoke")
    coil_count = lax.axis_size("coil")
    slab_rows = grid_len // slab_count
    block_len = slab_rows + 2 * REACH
    columns = coil_dev * part_count * kz_len
    group = slab_count * slot_count
    depth = block_len * group

    live_flag = (jnp.arange(slot_count, dtype=jnp.int32) < live_count[0]).astype(jnp.float32)
    table_hit = dcf_index[:, :, None] == jnp.arange(dcf_table.shape[0], dtype=jnp.int32)[None, None, :]
    density = jnp.sum(jnp.where(table_hit, dcf_table[None, None, :], 0.0), axis=2) * live_flag[:, None]

    picked = slab_owner[:, None] * slab_rows + jnp.arange(block_len, dtype=jnp.int32)[None, :]
    geometry = jnp.stack([coords[:, 0], coords[:, 1], density], axis=0)
    geometry = jnp.pad(geometry, ((0, 0), (0, 0), (REACH, REACH)))
    geometry = jnp.take(geometry, picked, axis=2)
    starts = jnp.broadcast_to(
        jnp.take(foot_offset, slab_owner, axis=1).astype(jnp.float32)[None, :, :, None],
        (1, slot_count, slab_count, block_len),
    )
    geometry = jnp.transpose(jnp.concatenate([geometry, starts], axis=0), (2, 0, 3, 1))
    got_geometry = lax.all_to_all(geometry, "spoke", split_axis=0, concat_axis=0, tiled=True)
    got_geometry = jnp.transpose(got_geometry, (1, 2, 0, 3)).reshape(4, depth)

    samples = kdata.reshape(slot_count, columns, grid_len)
    turned = sum(
        jnp.einsum("tcs,cd->std", samples, table, preferred_element_type=jnp.float32) for table in depth_tables
    ).astype(jnp.bfloat16)
    turned = jnp.pad(turned, ((REACH, REACH), (0, 0), (0, 0)))
    blocks = jnp.take(turned, picked, axis=0)
    got = lax.all_to_all(blocks, "spoke", split_axis=0, concat_axis=0, tiled=True)
    got = jnp.transpose(got, (1, 0, 2, 3)).reshape(depth, columns)

    owned_slab = slab_owner[lax.axis_index("spoke")].reshape(1)
    rows_step = min(ROWS_STEP, slab_rows)
    whole = lambda shape: pl.BlockSpec(shape, lambda step: (0,) * len(shape))
    images, power = pl.pallas_call(
        functools.partial(slab_kernel, group=group),
        grid=(slab_rows // rows_step,),
        in_specs=[
            pl.BlockSpec(memory_space=pltpu.SMEM),
            whole((depth, columns)),
            whole((4, depth)),
            whole((2 * grid_len, 2 * grid_len)),
            whole((2 * grid_len, 2 * grid_len)),
        ],
        out_specs=[
            pl.BlockSpec((rows_step, coil_dev, part_count, kz_len, grid_len), lambda step: (step, 0, 0, 0, 0)),
            pl.BlockSpec((rows_step, kz_len, grid_len), lambda step: (step, 0, 0)),
        ],
        out_shape=[
            jax.ShapeDtypeStruct((slab_rows, coil_dev, part_count, kz_len, grid_len), jnp.float32),
            jax.ShapeDtypeStruct((slab_rows, kz_len, grid_len), jnp.bfloat16),
        ],
        scratch_shapes=[
            pltpu.VMEM((columns, depth), jnp.bfloat16),
            pltpu.VMEM((grid_len, depth), jnp.float32),
            pltpu.VMEM((slab_rows, depth), jnp.float32),
        ],
        compiler_params=pltpu.CompilerParams(dimension_semantics=("arbitrary",)),
    )(owned_slab, got, got_geometry, *column_tables)

    power = lax.all_to_all(power, "coil", split_axis=1, concat_axis=0, tiled=True)
    power = power.reshape(coil_count, slab_rows, kz_len // coil_count, grid_len)
    combined = jnp.sqrt(jnp.sum(power.astype(jnp.float32), axis=0))
    return (images, combined)


def solution(mesh):
    def run(kdata, *rest):
        coil_dev = kdata.shape[1] // mesh.shape["coil"]
        depth_tables = two_terms(np.kron(np.eye(coil_dev), inverse_matrix(kdata.shape[3])))
        column_tables = two_terms(inverse_matrix(kdata.shape[4]))
        return jax.shard_map(
            functools.partial(on_device, depth_tables, column_tables),
            mesh=mesh,
            in_specs=(
                P("spoke", "coil", None, None, None),
                P("spoke", None, None),
                P("spoke", None),
                P("spoke"),
                P(),
                P("spoke", None),
                P(),
            ),
            out_specs=(P("spoke", "coil", None, None, None), P("spoke", "coil", None)),
            check_vma=False,
        )(kdata, *rest)

    return run
```

```python
import functools
import math

import jax
import jax.numpy as jnp
import numpy as np
from jax import lax
from jax.experimental import pallas as pl
from jax.experimental.pallas import tpu as pltpu
from jax.sharding import PartitionSpec as P

FW = 32
REACH = 2
ROWS_STEP = 4


def kernel(distance):
    inner = jnp.maximum(1.0 - distance * distance * 0.25, 0.0)
    return inner * inner


def inverse_matrix(length):
    counter = np.arange(length)
    phase = 2.0 * np.pi / length * (counter[:, None] * counter[None, :] % length)
    cosine = np.cos(phase) / math.sqrt(length)
    sine = np.sin(phase) / math.sqrt(length)
    return np.block([[cosine, sine], [-sine, cosine]])


def two_terms(table):
    high = table.astype(jnp.bfloat16)
    low = (table - high.astype(np.float64)).astype(jnp.bfloat16)
    return high, low


def slab_kernel(place_ref, geometry_ref, high_ref, low_ref, *refs, group, value_count, alias_count):
    value_refs = refs[:value_count]
    image_ref, keep_ref, send_ref, turned_ref, col_ref, row_ref = refs[value_count + alias_count :]
    step = pl.program_id(0)
    rows_step, coil_dev, _, kz_len, grid_len = image_ref.shape
    chunk_rows, depth = row_ref.shape
    kz_part = keep_ref.shape[2]

    @pl.when(step == 0)
    def _():
        first_row = place_ref[0]
        chunk = 2 * group
        samples = [(ref, index) for ref in value_refs for index in range(ref.shape[1])]
        for start in range(0, depth, chunk):
            part = slice(start, start + chunk)
            taken = samples[start // group : start // group + 2]
            taken = [ref[:, index].reshape(group, ref.shape[3]) for ref, index in taken]
            turned_ref[:, part] = jnp.concatenate(taken, axis=0).T
            geometry = geometry_ref[:, part]
            cells = lax.broadcasted_iota(jnp.int32, (grid_len, chunk), 0).astype(jnp.float32)
            begin = geometry[3:4]
            covered = (cells >= begin) & (cells < begin + FW)
            col_ref[:, part] = jnp.where(covered, kernel(cells + 0.5 - geometry[1:2]), 0.0)
            rows = (first_row + lax.broadcasted_iota(jnp.int32, (chunk_rows, chunk), 0)).astype(jnp.float32)
            row_ref[:, part] = geometry[2:3] * kernel(rows + 0.5 - geometry[0:1])

    span = (2 + 2 * REACH) * group
    pieces = []
    for pair in range(rows_step // 2):
        row = step * rows_step + 2 * pair
        lanes = pl.ds(pl.multiple_of(row * group, 128), span)
        values = turned_ref[:, lanes]
        columns = col_ref[:, lanes]
        for half in range(2):
            weight = (row_ref[pl.ds(row + half, 1), lanes] * columns).astype(jnp.bfloat16)
            cells = lax.dot_general(
                values, weight, (((1,), (1,)), ((), ())), preferred_element_type=jnp.float32
            ).astype(jnp.bfloat16)
            for coil in range(coil_dev):
                base = coil * 2 * kz_len
                pieces.append(
                    jnp.concatenate([cells[base : base + kz_len], cells[base + kz_len : base + 2 * kz_len]], axis=1)
                )
    stacked = jnp.concatenate(pieces, axis=0)
    out = jnp.dot(stacked, high_ref[...], preferred_element_type=jnp.float32)
    out = out + jnp.dot(stacked, low_ref[...], preferred_element_type=jnp.float32)
    first_core = place_ref[1] == 0
    for row in range(rows_step):
        power = jnp.zeros((kz_len, grid_len), jnp.float32)
        for coil in range(coil_dev):
            base = (row * coil_dev + coil) * kz_len
            for part in range(2):
                image = out[base : base + kz_len, part * grid_len : (part + 1) * grid_len]
                image_ref[row, coil, part] = image
                power = power + image * image
        for chip in range(keep_ref.shape[0]):
            one = power[2 * chip * kz_part : (2 * chip + 1) * kz_part]
            two = power[(2 * chip + 1) * kz_part : (2 * chip + 2) * kz_part]
            keep_ref[chip, row] = jnp.where(first_core, one, two)
            send_ref[chip, row] = jnp.where(first_core, two, one).astype(send_ref.dtype)


def image_chunk(done, place, values, geometry, column_tables, shape, first, rows, chips):
    slab_rows, coil_dev, part_count, kz_len, grid_len = shape
    depth = geometry.shape[1]
    columns = coil_dev * part_count * kz_len
    slab_count, _, slot_count, _ = values[0][0].shape
    group = slab_count * slot_count
    kz_part = kz_len // (2 * chips)
    offset = first // ROWS_STEP
    whole = lambda size: pl.BlockSpec(size, lambda step: (0,) * len(size))
    samples = lambda count, at: pl.BlockSpec((slab_count, count, slot_count, columns), lambda step: (0, at, 0, 0))
    halves = pl.BlockSpec((chips, ROWS_STEP, kz_part, grid_len), lambda step: (0, step + offset, 0, 0))
    macs = rows * columns * grid_len * (6 * group + 4 * grid_len)
    return pl.pallas_call(
        functools.partial(slab_kernel, group=group, value_count=len(values), alias_count=len(done)),
        grid=(rows // ROWS_STEP,),
        in_specs=[
            pl.BlockSpec(memory_space=pltpu.SMEM),
            whole((4, depth)),
            whole((2 * grid_len, 2 * grid_len)),
            whole((2 * grid_len, 2 * grid_len)),
        ]
        + [samples(count, at) for _, count, at in values]
        + [pl.BlockSpec(memory_space=pl.ANY)] * len(done),
        out_specs=[
            pl.BlockSpec((ROWS_STEP, coil_dev, part_count, kz_len, grid_len), lambda step: (step + offset, 0, 0, 0, 0)),
            halves,
            halves,
        ],
        out_shape=[
            jax.ShapeDtypeStruct(shape, jnp.float32),
            jax.ShapeDtypeStruct((chips, slab_rows, kz_part, grid_len), jnp.float32),
            jax.ShapeDtypeStruct((chips, slab_rows, kz_part, grid_len), jnp.bfloat16),
        ],
        scratch_shapes=[
            pltpu.VMEM((columns, depth), jnp.bfloat16),
            pltpu.VMEM((grid_len, depth), jnp.float32),
            pltpu.VMEM((rows, depth), jnp.float32),
        ],
        input_output_aliases={4 + len(values) + i: i for i in range(len(done))},
        cost_estimate=pl.CostEstimate(
            flops=2 * macs, bytes_accessed=rows * columns * grid_len * 4, transcendentals=0
        ),
        compiler_params=pltpu.CompilerParams(dimension_semantics=("arbitrary",)),
    )(place, geometry, *column_tables, *[array for array, _, _ in values], *done)


def coil_sum(keep, send, chips):
    count = 2 * chips
    me = lax.axis_index("coil")
    chip = me // 2
    got = lax.ppermute(send, "coil", [(i, i ^ 1) for i in range(count)])
    both = keep + got.astype(jnp.float32)
    total = lax.dynamic_index_in_dim(both, chip, 0, keepdims=False)
    for turn in range(1, chips):
        block = lax.dynamic_index_in_dim(both, (chip + turn) % chips, 0, keepdims=False).astype(jnp.bfloat16)
        got = lax.ppermute(block, "coil", [(i, (i + 2 * turn) % count) for i in range(count)])
        total = total + got.astype(jnp.float32)
    return jnp.sqrt(total)


def on_device(depth_tables, column_tables, kdata, coords, foot_offset, live_count, dcf_table, dcf_index, slab_owner):
    slot_count, coil_dev, part_count, kz_len, grid_len = kdata.shape
    slab_count = lax.axis_size("spoke")
    chips = lax.axis_size("coil") // 2
    slab_rows = grid_len // slab_count
    block_len = slab_rows + 2 * REACH
    columns = coil_dev * part_count * kz_len
    group = slab_count * slot_count
    second = max(ROWS_STEP, slab_rows * 3 // 8 // ROWS_STEP * ROWS_STEP)
    first = slab_rows - second
    edge = first + 2 * REACH

    samples = kdata.reshape(slot_count, columns, grid_len)
    turned = sum(
        jnp.einsum("tcs,cd->std", samples, table, preferred_element_type=jnp.float32) for table in depth_tables
    ).astype(jnp.bfloat16)
    turned = jnp.pad(turned, ((REACH, REACH), (0, 0), (0, 0)))
    picked = slab_owner[:, None] * slab_rows + jnp.arange(block_len, dtype=jnp.int32)[None, :]
    sent = [jnp.take(turned, part, axis=0, mode="clip") for part in (picked[:, :edge], picked[:, edge:])]
    got_first = lax.all_to_all(sent[0], "spoke", split_axis=0, concat_axis=0, tiled=True)
    got_second = lax.all_to_all(sent[1], "spoke", split_axis=0, concat_axis=0, tiled=True)

    coords, dcf_index, _ = lax.optimization_barrier((coords, dcf_index, sent[0]))
    live_flag = (jnp.arange(slot_count, dtype=jnp.int32) < live_count[0]).astype(jnp.float32)
    table_hit = dcf_index[:, :, None] == jnp.arange(dcf_table.shape[0], dtype=jnp.int32)[None, None, :]
    density = jnp.sum(jnp.where(table_hit, dcf_table[None, None, :], 0.0), axis=2) * live_flag[:, None]
    starts = jnp.pad(foot_offset.astype(jnp.float32), ((0, 0), (0, grid_len - slab_count)))
    geometry = jnp.stack([coords[:, 0], coords[:, 1], density, starts], axis=0)
    geometry = lax.all_gather(geometry, "spoke", axis=1, tiled=True)

    owned_slab = slab_owner[lax.axis_index("spoke")]
    first_row = owned_slab * slab_rows
    starts = lax.dynamic_slice(geometry, (3, 0, owned_slab), (1, group, 1))
    near = lax.dynamic_slice_in_dim(
        jnp.pad(geometry[:3], ((0, 0), (0, 0), (REACH, REACH))), first_row, block_len, axis=2
    )
    geometry = jnp.concatenate([near, jnp.broadcast_to(starts, (1, group, block_len))], axis=0)
    geometry = jnp.transpose(geometry, (0, 2, 1)).reshape(4, block_len * group)

    core = lax.axis_index("coil") % 2
    place = jnp.stack([first_row, core]).astype(jnp.int32)
    shape = (slab_rows, coil_dev, part_count, kz_len, grid_len)
    done = image_chunk(
        (), place, [(got_first, edge, 0)], geometry[:, : edge * group], column_tables, shape, 0, first, chips
    )
    place = jnp.stack([first_row + first, core]).astype(jnp.int32)
    values = [(got_first, 2 * REACH, first // (2 * REACH)), (got_second, second, 0)]
    images, keep, send = image_chunk(
        done, place, values, geometry[:, first * group :], column_tables, shape, first, second, chips
    )
    return (images, coil_sum(keep, send, chips))


def solution(mesh):
    def run(kdata, *rest):
        coil_dev = kdata.shape[1] // mesh.shape["coil"]
        depth_tables = two_terms(np.kron(np.eye(coil_dev), inverse_matrix(kdata.shape[3])))
        column_tables = two_terms(inverse_matrix(kdata.shape[4]))
        return jax.shard_map(
            functools.partial(on_device, depth_tables, column_tables),
            mesh=mesh,
            in_specs=(
                P("spoke", "coil", None, None, None),
                P("spoke", None, None),
                P("spoke", None),
                P("spoke"),
                P(),
                P("spoke", None),
                P(),
            ),
            out_specs=(P("spoke", "coil", None, None, None), P("spoke", "coil", None)),
            check_vma=False,
        )(kdata, *rest)

    return run
```

```python
import functools
import math

import jax
import jax.numpy as jnp
import numpy as np
from jax import lax
from jax.experimental import pallas as pl
from jax.experimental.pallas import tpu as pltpu
from jax.sharding import PartitionSpec as P

FW = 32
REACH = 2
ROWS_STEP = 4


def kernel(distance):
    inner = jnp.maximum(1.0 - distance * distance * 0.25, 0.0)
    return inner * inner


def inverse_matrix(length):
    counter = np.arange(length)
    phase = 2.0 * np.pi / length * (counter[:, None] * counter[None, :] % length)
    cosine = np.cos(phase) / math.sqrt(length)
    sine = np.sin(phase) / math.sqrt(length)
    return np.block([[cosine, sine], [-sine, cosine]])


def two_terms(table):
    high = table.astype(jnp.bfloat16)
    low = (table - high.astype(np.float64)).astype(jnp.bfloat16)
    return high, low


def slab_kernel(place_ref, geometry_ref, high_ref, low_ref, *refs, group, value_count, alias_count):
    value_refs = refs[:value_count]
    image_ref, keep_ref, send_ref, turned_ref, col_ref, row_ref = refs[value_count + alias_count :]
    step = pl.program_id(0)
    rows_step, coil_dev, _, kz_len, grid_len = image_ref.shape
    chunk_rows, depth = row_ref.shape
    kz_part = keep_ref.shape[2]

    @pl.when(step == 0)
    def _():
        first_row = place_ref[0]
        chunk = 2 * group
        samples = [(ref, index) for ref in value_refs for index in range(ref.shape[1])]
        for start in range(0, depth, chunk):
            part = slice(start, start + chunk)
            taken = samples[start // group : start // group + 2]
            taken = [ref[:, index].reshape(group, ref.shape[3]) for ref, index in taken]
            turned_ref[:, part] = jnp.concatenate(taken, axis=0).T
            geometry = geometry_ref[:, part]
            cells = lax.broadcasted_iota(jnp.int32, (grid_len, chunk), 0).astype(jnp.float32)
            begin = geometry[3:4]
            covered = (cells >= begin) & (cells < begin + FW)
            col_ref[:, part] = jnp.where(covered, kernel(cells + 0.5 - geometry[1:2]), 0.0)
            rows = (first_row + lax.broadcasted_iota(jnp.int32, (chunk_rows, chunk), 0)).astype(jnp.float32)
            row_ref[:, part] = geometry[2:3] * kernel(rows + 0.5 - geometry[0:1])

    span = (2 + 2 * REACH) * group
    pieces = []
    for pair in range(rows_step // 2):
        row = step * rows_step + 2 * pair
        lanes = pl.ds(pl.multiple_of(row * group, 128), span)
        values = turned_ref[:, lanes]
        columns = col_ref[:, lanes]
        for half in range(2):
            weight = (row_ref[pl.ds(row + half, 1), lanes] * columns).astype(jnp.bfloat16)
            cells = lax.dot_general(
                values, weight, (((1,), (1,)), ((), ())), preferred_element_type=jnp.float32
            ).astype(jnp.bfloat16)
            for coil in range(coil_dev):
                base = coil * 2 * kz_len
                pieces.append(
                    jnp.concatenate([cells[base : base + kz_len], cells[base + kz_len : base + 2 * kz_len]], axis=1)
                )
    stacked = jnp.concatenate(pieces, axis=0)
    out = jnp.dot(stacked, high_ref[...], preferred_element_type=jnp.float32)
    out = out + jnp.dot(stacked, low_ref[...], preferred_element_type=jnp.float32)
    first_core = place_ref[1] == 0
    for row in range(rows_step):
        power = jnp.zeros((kz_len, grid_len), jnp.float32)
        for coil in range(coil_dev):
            base = (row * coil_dev + coil) * kz_len
            for part in range(2):
                image = out[base : base + kz_len, part * grid_len : (part + 1) * grid_len]
                image_ref[row, coil, part] = image
                power = power + image * image
        for chip in range(keep_ref.shape[0]):
            one = power[2 * chip * kz_part : (2 * chip + 1) * kz_part]
            two = power[(2 * chip + 1) * kz_part : (2 * chip + 2) * kz_part]
            keep_ref[chip, row] = jnp.where(first_core, one, two)
            send_ref[chip, row] = jnp.where(first_core, two, one).astype(send_ref.dtype)


def image_chunk(done, place, values, geometry, column_tables, shape, first, rows, chips):
    slab_rows, coil_dev, part_count, kz_len, grid_len = shape
    depth = geometry.shape[1]
    columns = coil_dev * part_count * kz_len
    slab_count, _, slot_count, _ = values[0][0].shape
    group = slab_count * slot_count
    kz_part = kz_len // (2 * chips)
    offset = first // ROWS_STEP
    whole = lambda size: pl.BlockSpec(size, lambda step: (0,) * len(size))
    samples = lambda count, at: pl.BlockSpec((slab_count, count, slot_count, columns), lambda step: (0, at, 0, 0))
    halves = pl.BlockSpec((chips, ROWS_STEP, kz_part, grid_len), lambda step: (0, step + offset, 0, 0))
    macs = rows * columns * grid_len * (6 * group + 4 * grid_len)
    return pl.pallas_call(
        functools.partial(slab_kernel, group=group, value_count=len(values), alias_count=len(done)),
        grid=(rows // ROWS_STEP,),
        in_specs=[
            pl.BlockSpec(memory_space=pltpu.SMEM),
            whole((4, depth)),
            whole((2 * grid_len, 2 * grid_len)),
            whole((2 * grid_len, 2 * grid_len)),
        ]
        + [samples(count, at) for _, count, at in values]
        + [pl.BlockSpec(memory_space=pl.ANY)] * len(done),
        out_specs=[
            pl.BlockSpec((ROWS_STEP, coil_dev, part_count, kz_len, grid_len), lambda step: (step + offset, 0, 0, 0, 0)),
            halves,
            halves,
        ],
        out_shape=[
            jax.ShapeDtypeStruct(shape, jnp.float32),
            jax.ShapeDtypeStruct((chips, slab_rows, kz_part, grid_len), jnp.float32),
            jax.ShapeDtypeStruct((chips, slab_rows, kz_part, grid_len), jnp.bfloat16),
        ],
        scratch_shapes=[
            pltpu.VMEM((columns, depth), jnp.bfloat16),
            pltpu.VMEM((grid_len, depth), jnp.float32),
            pltpu.VMEM((rows, depth), jnp.float32),
        ],
        input_output_aliases={4 + len(values) + i: i for i in range(len(done))},
        cost_estimate=pl.CostEstimate(
            flops=2 * macs, bytes_accessed=rows * columns * grid_len * 4, transcendentals=0
        ),
        compiler_params=pltpu.CompilerParams(dimension_semantics=("arbitrary",)),
    )(place, geometry, *column_tables, *[array for array, _, _ in values], *done)


def coil_sum(keep, send, chips):
    count = 2 * chips
    me = lax.axis_index("coil")
    chip = me // 2
    got = lax.ppermute(send, "coil", [(i, i ^ 1) for i in range(count)])
    both = keep + got.astype(jnp.float32)
    total = lax.dynamic_index_in_dim(both, chip, 0, keepdims=False)
    for turn in range(1, chips):
        block = lax.dynamic_index_in_dim(both, (chip + turn) % chips, 0, keepdims=False).astype(jnp.bfloat16)
        got = lax.ppermute(block, "coil", [(i, (i + 2 * turn) % count) for i in range(count)])
        total = total + got.astype(jnp.float32)
    return jnp.sqrt(total)


def on_device(depth_tables, column_tables, kdata, coords, foot_offset, live_count, dcf_table, dcf_index, slab_owner):
    slot_count, coil_dev, part_count, kz_len, grid_len = kdata.shape
    slab_count = lax.axis_size("spoke")
    chips = lax.axis_size("coil") // 2
    slab_rows = grid_len // slab_count
    block_len = slab_rows + 2 * REACH
    columns = coil_dev * part_count * kz_len
    group = slab_count * slot_count
    second = max(ROWS_STEP, slab_rows * 3 // 8 // ROWS_STEP * ROWS_STEP)
    first = slab_rows - second
    edge = first + 2 * REACH

    live_flag = (jnp.arange(slot_count, dtype=jnp.int32) < live_count[0]).astype(jnp.float32)
    table_hit = dcf_index[:, :, None] == jnp.arange(dcf_table.shape[0], dtype=jnp.int32)[None, None, :]
    density = jnp.sum(jnp.where(table_hit, dcf_table[None, None, :], 0.0), axis=2) * live_flag[:, None]

    picked = slab_owner[:, None] * slab_rows + jnp.arange(block_len, dtype=jnp.int32)[None, :]
    geometry = jnp.stack([coords[:, 0], coords[:, 1], density], axis=0)
    geometry = jnp.pad(geometry, ((0, 0), (0, 0), (REACH, REACH)))
    geometry = jnp.take(geometry, picked, axis=2, mode="clip")
    starts = jnp.broadcast_to(
        jnp.take(foot_offset, slab_owner, axis=1, mode="clip").astype(jnp.float32)[None, :, :, None],
        (1, slot_count, slab_count, block_len),
    )
    geometry = jnp.transpose(jnp.concatenate([geometry, starts], axis=0), (2, 0, 3, 1))
    got_geometry = lax.all_to_all(geometry, "spoke", split_axis=0, concat_axis=0, tiled=True)
    geometry = jnp.transpose(got_geometry, (1, 2, 0, 3)).reshape(4, block_len * group)

    samples = kdata.reshape(slot_count, columns, grid_len)
    turned = sum(
        jnp.einsum("tcs,cd->std", samples, table, preferred_element_type=jnp.float32) for table in depth_tables
    ).astype(jnp.bfloat16)
    turned = jnp.pad(turned, ((REACH, REACH), (0, 0), (0, 0)))
    sent = [jnp.take(turned, part, axis=0, mode="clip") for part in (picked[:, :edge], picked[:, edge:])]
    got_first = lax.all_to_all(sent[0], "spoke", split_axis=0, concat_axis=0, tiled=True)
    got_second = lax.all_to_all(sent[1], "spoke", split_axis=0, concat_axis=0, tiled=True)

    first_row = slab_owner[lax.axis_index("spoke")] * slab_rows
    core = lax.axis_index("coil") % 2
    place = jnp.stack([first_row, core]).astype(jnp.int32)
    shape = (slab_rows, coil_dev, part_count, kz_len, grid_len)
    done = image_chunk(
        (), place, [(got_first, edge, 0)], geometry[:, : edge * group], column_tables, shape, 0, first, chips
    )
    place = jnp.stack([first_row + first, core]).astype(jnp.int32)
    values = [(got_first, 2 * REACH, first // (2 * REACH)), (got_second, second, 0)]
    images, keep, send = image_chunk(
        done, place, values, geometry[:, first * group :], column_tables, shape, first, second, chips
    )
    return (images, coil_sum(keep, send, chips))


def solution(mesh):
    def run(kdata, *rest):
        coil_dev = kdata.shape[1] // mesh.shape["coil"]
        depth_tables = two_terms(np.kron(np.eye(coil_dev), inverse_matrix(kdata.shape[3])))
        column_tables = two_terms(inverse_matrix(kdata.shape[4]))
        return jax.shard_map(
            functools.partial(on_device, depth_tables, column_tables),
            mesh=mesh,
            in_specs=(
                P("spoke", "coil", None, None, None),
                P("spoke", None, None),
                P("spoke", None),
                P("spoke"),
                P(),
                P("spoke", None),
                P(),
            ),
            out_specs=(P("spoke", "coil", None, None, None), P("spoke", "coil", None)),
            check_vma=False,
        )(kdata, *rest)

    return run
```
